128 devices in a mesh: row: 8 (over x_hi, z), col: 8 (over y, x_lo), layer: 2 (over core).
Axes of the slice: x: 4 (x_hi: 2, x_lo: 2; x = x_hi * 2 + x_lo), y: 4, z: 4, core: 2. Of those that a mesh axis runs over, the one named last changes fastest.
Arguments:
- expression: bfloat16 [24576, 1024], P(('row', 'col'), 'layer'), may hold values from -240 to 240
Outputs:
- connectivity: float32 [24576], P(('row', 'col', 'layer'))
The draws below stay inside these ranges and needn't reach their ends.
All inputs are finite; a program needn't handle non-finite values.
Results may differ from the reference program's by a relative error of at most 0.00048.
Values may be sent and summed in bfloat16 or wider, within the bound.
No kernel may reach another device: no remote copies, remote signals or barrier semaphores. Data moves between devices by JAX's collectives and lax.ppermute only.
A program may use at most 64 MiB of HBM per device.

```python
import math
import jax
import jax.numpy as jnp
from jax import lax

S = 1024
G = 24576


module_count = 384


membership = 3


def draw_expression(key, part):
    keys = jax.random.split(key, 7)
    modules = jax.random.randint(keys[0], (G, membership), 0, module_count)
    loading = jax.random.uniform(keys[1], (G, membership), jnp.float32, -1.0, 1.0)
    factor = jax.random.truncated_normal(keys[2], -3.0, 3.0, (module_count, S), jnp.float32)
    white = jax.random.truncated_normal(keys[3], -4.0, 4.0, (G, S), jnp.float32)
    mixing = jax.random.truncated_normal(keys[6], -4.0, 4.0, (S, S), jnp.float32) / jnp.sqrt(jnp.float32(S))
    spread = jnp.exp(jax.random.uniform(keys[4], (G,), jnp.float32, jnp.log(0.5), jnp.log(2.0)))
    offset = jax.random.uniform(keys[5], (G,), jnp.float32, -3.0, 3.0)
    exponent = 0.3
    decay = (1.0 + jnp.arange(S).astype(jnp.float32)) ** (-exponent)
    decay = decay / jnp.sqrt(jnp.mean(decay * decay))
    noise = jnp.dot(white * decay[None, :], mixing, precision=lax.Precision.HIGHEST)
    noise = jnp.clip(noise, -5.0, 5.0)
    columns = jnp.arange(module_count)
    load_matrix = jnp.zeros((G, module_count), jnp.float32)
    for member in range(membership):
        picked = (modules[:, member][:, None] == columns[None, :]).astype(jnp.float32)
        load_matrix = load_matrix + picked * loading[:, member][:, None]
    signal = jnp.dot(load_matrix, factor, precision=lax.Precision.HIGHEST)
    weights = 1.0 + 2.0 * jnp.arange(S).astype(jnp.float32) / (S - 1)
    values = offset[:, None] + spread[:, None] * weights[None, :] * (noise + 1.5 * signal)
    return values.astype(jnp.bfloat16)


def setup_inputs(seed: int = 0) -> dict:
    key_of = jax.random.split(jax.random.key(seed), 2)
    return {
        "expression": draw_expression(jax.random.fold_in(key_of[1], 71), 0),
    }


epsilon = 1e-05

def adjacency(correlation):
    shifted = (1.0 + correlation) * 0.5
    square = shifted * shifted
    fourth = square * square
    eighth = fourth * fourth
    return eighth * fourth

def reference(expression):
    values = expression.astype(jnp.float32)
    total = lax.optimization_barrier(jnp.sum(values, axis=1))
    squares = lax.optimization_barrier(jnp.sum(values * values, axis=1))
    average = total / S
    variance = squares / S - average * average
    scaled = ((values - average[:, None]) * lax.rsqrt(variance + epsilon)[:, None]).astype(jnp.bfloat16)
    block_rows = math.gcd(G, 1024)
    grouped = scaled.reshape(G // block_rows, block_rows, S)

    def one_block(segment):
        tile_sum = lax.dot_general(segment, scaled, (((1,), (1,)), ((), ())), preferred_element_type=jnp.float32)
        return lax.optimization_barrier(jnp.sum(adjacency(tile_sum / S), axis=1))
    totals = lax.map(one_block, grouped).reshape(G)
    return totals - 1.0
```

```python
import itertools

import jax
import jax.numpy as jnp
from jax import lax
from jax.experimental import pallas as pl
from jax.experimental.pallas import tpu as pltpu
from jax.sharding import Mesh
from jax.sharding import PartitionSpec as P

S = 1024
N = 4
CHIP = ("x_hi", "z", "y", "x_lo")
ALL = CHIP + ("layer",)
epsilon = 1e-05


OFFSETS = (
    ((0, 0, 0), None),
    ((1, 0, 1), None),
    ((3, 1, 0), None),
    ((0, 3, 3), None),
    ((0, 3, 0), None),
    ((0, 0, 1), None),
    ((0, 0, 3), None),
    ((2, 0, 1), (1, 0, 1)),
    ((2, 1, 0), (3, 1, 0)),
    ((0, 2, 3), (0, 3, 3)),
    ((3, 1, 3), (3, 1, 0)),
)
DELTA = tuple(d for d, _ in OFFSETS)
BLOCKS = len(DELTA)


def minus(a, b):
    return tuple((p - q) % N for p, q in zip(a, b))


def choose_pairs():
    pairs, done = [(0, 0, False)], {(0, 0, 0)}
    for j, i in itertools.product(range(BLOCKS), range(BLOCKS)):
        if i >= j:
            continue
        d = minus(DELTA[i], DELTA[j])
        if d not in done:
            e = minus((0, 0, 0), d)
            done |= {d, e}
            pairs.append((i, j, d != e))
    assert len(done) == N**3
    return tuple(pairs)


PAIRS = choose_pairs()


def place(x, y, z, c):
    return (((x // 2 * N + z) * N + y) * 2 + x % 2) * 2 + c


def chips():
    return itertools.product(range(N), range(N), range(N))


def fetch(value, d, flip=0):
    pairs = []
    for p in chips():
        q = tuple((a + b) % N for a, b in zip(p, d))
        for c in range(2):
            pairs.append((place(*q, c ^ flip), place(*p, c)))
    return lax.ppermute(value, ALL, pairs)


def deliver(value, d0, d1):
    pairs = []
    for p in chips():
        for c, d in enumerate((d0, d1)):
            q = tuple((a + b) % N for a, b in zip(p, d))
            pairs.append((place(*p, c), place(*q, c)))
    return lax.ppermute(value, ALL, pairs)


def partial_sums(*refs):
    raw, (out_ref, x_ref, row_ref, col_ref) = refs[: 2 * BLOCKS], refs[2 * BLOCKS :]
    core = lax.axis_index("layer")
    genes = x_ref.shape[1]
    half = genes // 2
    for b in range(BLOCKS):
        lo = raw[2 * b][...].astype(jnp.float32)
        hi = raw[2 * b + 1][...].astype(jnp.float32)
        total = jnp.sum(lo, axis=1, keepdims=True) + jnp.sum(hi, axis=1, keepdims=True)
        squares = jnp.sum(lo * lo, axis=1, keepdims=True) + jnp.sum(
            hi * hi, axis=1, keepdims=True
        )
        average = total / S
        variance = squares / S - average * average
        scale = lax.rsqrt(variance + epsilon)
        x_ref[b, :, : S // 2] = (((lo - average) * scale) * 0.03125).astype(jnp.bfloat16)
        x_ref[b, :, S // 2 :] = (((hi - average) * scale) * 0.03125).astype(jnp.bfloat16)
    row_ref[...] = jnp.zeros_like(row_ref)
    col_ref[...] = jnp.zeros_like(col_ref)
    mine = pl.ds(pl.multiple_of(core * half, half), half)
    for i, j, both in PAIRS:
        t = lax.dot_general(
            x_ref[j],
            x_ref[i, mine, :],
            (((1,), (1,)), ((), ())),
            preferred_element_type=jnp.float32,
        )
        t = 1.0 + t
        t = t * t
        t = t * t
        t = t * t * t
        col_ref[i] += jnp.sum(t.reshape(genes // 8, 8, half), axis=0)
        if both:
            row_ref[j] += t[:, :128]
            row_ref[j, :, : half - 128] += t[:, 128:]
    ones = jnp.ones((8, 128), jnp.float32)
    for b in range(BLOCKS):
        rows = lax.dot_general(
            ones,
            row_ref[b],
            (((1,), (1,)), ((), ())),
            precision=lax.Precision.HIGHEST,
            preferred_element_type=jnp.float32,
        )
        cols = jnp.sum(col_ref[b], axis=0, keepdims=True)
        for h in range(2):
            here = jnp.where(core == h, cols, 0.0)
            out_ref[h, pl.ds(b, 1), :] = (rows[:1, h * half : (h + 1) * half] + here) * (0.5**12)


def on_device(expression):
    genes, samples = expression.shape
    half = genes // 2
    got = {}
    for d, parent in OFFSETS[1:]:
        got[d] = fetch(expression, d) if parent is None else fetch(got[parent], minus(d, parent))
    raw = []
    for d in DELTA:
        block = got.get(d, expression)
        raw += [block, fetch(block, (0, 0, 0), 1)]
    vmem = pl.BlockSpec(memory_space=pltpu.VMEM)
    sums = pl.pallas_call(
        partial_sums,
        out_shape=jax.ShapeDtypeStruct((2, 16, half), jnp.float32),
        in_specs=[vmem] * len(raw),
        out_specs=vmem,
        scratch_shapes=[
            pltpu.VMEM((BLOCKS, genes, S), jnp.bfloat16),
            pltpu.VMEM((BLOCKS, genes, 128), jnp.float32),
            pltpu.VMEM((BLOCKS, 8, half), jnp.float32),
        ],
        compiler_params=pltpu.CompilerParams(vmem_limit_bytes=60 * 2**20),
        name="partial_sums",
    )(*raw)
    first = lax.axis_index("layer") == 0
    own, set0, set1 = sums[:, 0], sums[:, 1:6], sums[:, 6:11]
    keep, give = jnp.where(first, set0, set1), jnp.where(first, set1, set0)
    keep = keep + fetch(give, (0, 0, 0), 1)
    arrived = [deliver(keep[:, m], DELTA[1 + m], DELTA[6 + m]) for m in range(5)]
    own = own + sum(arrived)
    mine, other = jnp.where(first, own[0], own[1]), jnp.where(first, own[1], own[0])
    return mine + fetch(other, (0, 0, 0), 1) - 1.0


def solution(mesh):
    torus = Mesh(mesh.devices.reshape(2, N, N, 2, 2), ALL)
    return jax.shard_map(
        on_device, mesh=torus, in_specs=(P(CHIP, "layer"),), out_specs=P(ALL), check_vma=False
    )
```

```python
import functools
import itertools

import jax
import jax.numpy as jnp
from jax import lax
from jax.experimental import pallas as pl
from jax.experimental.pallas import tpu as pltpu
from jax.sharding import Mesh
from jax.sharding import PartitionSpec as P


S = 1024
N = 4
CHIP = ("x_hi", "z", "y", "x_lo")
ALL = CHIP + ("layer",)
epsilon = 1e-05
VMEM_BYTES = 16 * 2**20


OFFSETS = (
    ((0, 0, 0), None),
    ((1, 0, 1), None),
    ((3, 1, 0), None),
    ((0, 3, 3), None),
    ((0, 3, 0), None),
    ((0, 0, 1), None),
    ((0, 0, 3), None),
    ((2, 0, 1), (1, 0, 1)),
    ((2, 1, 0), (3, 1, 0)),
    ((0, 2, 3), (0, 3, 3)),
    ((3, 1, 3), (3, 1, 0)),
)
DELTA = tuple(d for d, _ in OFFSETS)
BLOCKS = len(DELTA)


def minus(a, b):
    return tuple((p - q) % N for p, q in zip(a, b))


def choose_pairs():
    pairs, done = [(0, 0, False)], {(0, 0, 0)}
    for j, i in itertools.product(range(BLOCKS), range(BLOCKS)):
        if i >= j:
            continue
        d = minus(DELTA[i], DELTA[j])
        if d not in done:
            e = minus((0, 0, 0), d)
            done |= {d, e}
            pairs.append((i, j, d != e))
    assert len(done) == N**3
    return tuple(pairs)


PAIRS = choose_pairs()


def place(x, y, z, c):
    return (((x // 2 * N + z) * N + y) * 2 + x % 2) * 2 + c


def chips():
    return itertools.product(range(N), range(N), range(N))


def fetch(value, d, flip=0):
    pairs = []
    for p in chips():
        q = tuple((a + b) % N for a, b in zip(p, d))
        for c in range(2):
            pairs.append((place(*q, c ^ flip), place(*p, c)))
    return lax.ppermute(value, ALL, pairs)


def deliver(value, d0, d1):
    pairs = []
    for p in chips():
        for c, d in enumerate((d0, d1)):
            q = tuple((a + b) % N for a, b in zip(p, d))
            pairs.append((place(*p, c), place(*q, c)))
    return lax.ppermute(value, ALL, pairs)


def stage_sums(old, new, pairs, last, *refs):
    refs = list(refs)
    raw = [(refs.pop(0), refs.pop(0)) for _ in new]
    where = {b: refs.pop(0) for b in old}
    before = refs.pop(0) if old else None
    if last:
        own_ref, keep_ref, give_ref = refs.pop(0), refs.pop(0), refs.pop(0)
    else:
        out_ref = refs.pop(0)
    where |= {b: refs.pop(0) for b in new}
    row_ref, col_ref = refs
    core = lax.axis_index("layer")
    genes = raw[0][0].shape[0]
    half = genes // 2
    mine = pl.ds(pl.multiple_of(core * half, half), half)
    for b, (lo_ref, hi_ref) in zip(new, raw):
        lo = lo_ref[...].astype(jnp.float32)
        hi = hi_ref[...].astype(jnp.float32)
        total = jnp.sum(lo, axis=1, keepdims=True) + jnp.sum(hi, axis=1, keepdims=True)
        squares = jnp.sum(lo * lo, axis=1, keepdims=True) + jnp.sum(
            hi * hi, axis=1, keepdims=True
        )
        average = total / S
        variance = squares / S - average * average
        scale = lax.rsqrt(variance + epsilon)
        where[b][:, : S // 2] = (((lo - average) * scale) * 0.03125).astype(jnp.bfloat16)
        where[b][:, S // 2 :] = (((hi - average) * scale) * 0.03125).astype(jnp.bfloat16)
    rows_of = sorted({j for _, j, both in pairs if both})
    cols_of = sorted({i for i, _, _ in pairs})
    begun = set()
    for i, j, both in pairs:
        t = lax.dot_general(
            where[j][...],
            where[i][mine, :],
            (((1,), (1,)), ((), ())),
            preferred_element_type=jnp.float32,
        )
        t = 1.0 + t
        t = t * t
        t = t * t
        t = t * t * t
        cols = jnp.sum(t.reshape(genes // 8, 8, half), axis=0)
        c = cols_of.index(i)
        if ("c", i) in begun:
            col_ref[c] += cols
        else:
            col_ref[c] = cols
            begun.add(("c", i))
        if both:
            r = rows_of.index(j)
            wide = jnp.concatenate(
                [t[:, 128:], jnp.zeros((genes, 256 - half), jnp.float32)], axis=1
            )
            part = t[:, :128] + wide
            if ("r", j) in begun:
                row_ref[r] += part
            else:
                row_ref[r] = part
                begun.add(("r", j))
    ones = jnp.ones((8, 128), jnp.float32)
    for b in range(BLOCKS):
        parts = [jnp.zeros((1, half), jnp.float32)] * 2
        if before is not None:
            parts = [before[h, pl.ds(b, 1), :] for h in range(2)]
        if b in rows_of:
            rows = lax.dot_general(
                ones,
                row_ref[rows_of.index(b)],
                (((1,), (1,)), ((), ())),
                precision=lax.Precision.HIGHEST,
                preferred_element_type=jnp.float32,
            )
            parts = [p + rows[:1, h * half : (h + 1) * half] for h, p in enumerate(parts)]
        if b in cols_of:
            cols = jnp.sum(col_ref[cols_of.index(b)], axis=0, keepdims=True)
            parts = [p + jnp.where(core == h, cols, 0.0) for h, p in enumerate(parts)]
        for h in range(2):
            if not last:
                out_ref[h, pl.ds(b, 1), :] = parts[h]
            elif b == 0:
                own_ref[pl.ds(h, 1), :] = parts[h] * (0.5**12)
            else:
                kept = jnp.where(core == (b - 1) // 5, 1.0, 0.0) * (0.5**12)
                row = pl.ds((b - 1) % 5, 1)
                if b <= 5:
                    keep_ref[h, row, :] = parts[h] * kept
                    give_ref[h, row, :] = parts[h] * (0.5**12 - kept)
                else:
                    keep_ref[h, row, :] += parts[h] * kept
                    give_ref[h, row, :] += parts[h] * (0.5**12 - kept)


def joined_sums(keep_ref, got_ref, *out_refs):
    for m, out_ref in enumerate(out_refs):
        for h in range(2):
            row = pl.ds(m, 1)
            out_ref[pl.ds(h, 1), :] = keep_ref[h, row, :] + got_ref[h, row, :]


def owner_sums(own_ref, *refs):
    *arrived, mine_ref, other_ref = refs
    total = own_ref[...]
    for ref in arrived:
        total += ref[...]
    first = lax.axis_index("layer") == 0
    mine_ref[...] = jnp.where(first, total[:1], total[1:])
    other_ref[...] = jnp.where(first, total[1:], total[:1])


STAGES = ((0, 1, 2, 3), (4, 5, 6), (7, 8, 9, 10))


def all_sums(raw, genes):
    half = genes // 2
    vmem = pl.BlockSpec(memory_space=pltpu.VMEM)
    held, sums, old = [], [], []
    for number, new in enumerate(STAGES):
        last = number == len(STAGES) - 1
        have = old + list(new)
        pairs = [p for p in PAIRS if max(p[:2]) in new]
        assert all(i in have and j in have for i, j, _ in pairs)
        args = [h for b in new for h in raw[b]] + held + sums
        x_shape = ((genes, S), jnp.bfloat16)
        out_shape = [jax.ShapeDtypeStruct((2, 16, half), jnp.float32)]
        if last:
            out_shape = [jax.ShapeDtypeStruct((2, half), jnp.float32)]
            out_shape += [jax.ShapeDtypeStruct((2, 8, half), jnp.float32)] * 2
        scratch = [
            pltpu.VMEM((len({j for _, j, both in pairs if both}), genes, 128), jnp.float32),
            pltpu.VMEM((len({i for i, _, _ in pairs}), 8, half), jnp.float32),
        ]
        if last:
            scratch = [pltpu.VMEM(*x_shape) for _ in new] + scratch
        else:
            out_shape += [jax.ShapeDtypeStruct(*x_shape) for _ in new]
        call = pl.pallas_call(
            functools.partial(stage_sums, tuple(old), new, tuple(pairs), last),
            out_shape=out_shape,
            in_specs=[vmem] * len(args),
            out_specs=[vmem] * len(out_shape),
            scratch_shapes=scratch,
            compiler_params=pltpu.CompilerParams(vmem_limit_bytes=VMEM_BYTES),
            cost_estimate=pl.CostEstimate(
                flops=len(pairs) * genes * genes * S, bytes_accessed=2**20, transcendentals=0
            ),
        )
        done = call(*args)
        sums = [done[0]]
        held += done[1:]
        old += new
    return done


def small(body, results):
    vmem = pl.BlockSpec(memory_space=pltpu.VMEM)
    return pl.pallas_call(
        body,
        out_shape=[jax.ShapeDtypeStruct(r.shape, r.dtype) for r in results],
        out_specs=[vmem] * len(results),
        compiler_params=pltpu.CompilerParams(vmem_limit_bytes=2**20),
    )


def on_device(expression):
    genes, _ = expression.shape
    got = {DELTA[0]: expression}
    for d, parent in OFFSETS[1:]:
        source = expression if parent is None else got[parent]
        got[d] = fetch(source, d if parent is None else minus(d, parent))
    raw = []
    for d in DELTA:
        raw.append((got[d], fetch(got[d], (0, 0, 0), 1)))
    own, keep, give = all_sums(raw, genes)
    got = fetch(give, (0, 0, 0), 1)
    joined = small(joined_sums, [own] * 5)(keep, got)
    arrived = [deliver(v, DELTA[1 + m], DELTA[6 + m]) for m, v in enumerate(joined)]
    mine, other = small(owner_sums, [own[:1]] * 2)(own, *arrived)
    return (mine + fetch(other, (0, 0, 0), 1)).reshape(genes // 2) - 1.0


def solution(mesh):
    torus = Mesh(mesh.devices.reshape(2, N, N, 2, 2), ALL)

    return jax.shard_map(
        on_device, mesh=torus, in_specs=(P(CHIP, "layer"),), out_specs=P(ALL), check_vma=False
    )
```

```python
import functools
import itertools

import jax
import jax.numpy as jnp
from jax import lax
from jax.experimental import pallas as pl
from jax.experimental.pallas import tpu as pltpu
from jax.sharding import Mesh
from jax.sharding import PartitionSpec as P


S = 1024
N = 4
CHIP = ("x_hi", "z", "y", "x_lo")
ALL = CHIP + ("layer",)
epsilon = 1e-05
VMEM_BYTES = 16 * 2**20


OFFSETS = (
    ((0, 0, 0), None),
    ((1, 0, 3), None),
    ((3, 1, 0), None),
    ((0, 0, 1), None),
    ((0, 3, 0), None),
    ((2, 0, 3), (1, 0, 3)),
    ((2, 1, 0), (3, 1, 0)),
    ((3, 1, 3), (3, 1, 0)),
    ((0, 1, 0), None),
    ((0, 3, 1), (0, 0, 1)),
    ((0, 3, 2), (0, 3, 0)),
)
DELTA = tuple(d for d, _ in OFFSETS)
BLOCKS = len(DELTA)


def minus(a, b):
    return tuple((p - q) % N for p, q in zip(a, b))


def choose_pairs():
    pairs, done = [(0, 0, False)], {(0, 0, 0)}
    for j, i in itertools.product(range(BLOCKS), range(BLOCKS)):
        if i >= j:
            continue
        d = minus(DELTA[i], DELTA[j])
        if d not in done:
            e = minus((0, 0, 0), d)
            done |= {d, e}
            pairs.append((i, j, d != e))
    assert len(done) == N**3
    return tuple(pairs)


PAIRS = choose_pairs()


def place(x, y, z, c):
    return (((x // 2 * N + z) * N + y) * 2 + x % 2) * 2 + c


def chips():
    return itertools.product(range(N), range(N), range(N))


def fetch(value, d, flip=0):
    pairs = []
    for p in chips():
        q = tuple((a + b) % N for a, b in zip(p, d))
        for c in range(2):
            pairs.append((place(*q, c ^ flip), place(*p, c)))
    return lax.ppermute(value, ALL, pairs)


def deliver(value, d0, d1):
    pairs = []
    for p in chips():
        for c, d in enumerate((d0, d1)):
            q = tuple((a + b) % N for a, b in zip(p, d))
            pairs.append((place(*p, c), place(*q, c)))
    return lax.ppermute(value, ALL, pairs)


def standardize(own_ref, other_ref, own_out, other_out):
    rows = 32
    for r in range(0, own_ref.shape[0], rows):
        here = pl.ds(r, rows)
        own = own_ref[here, :].astype(jnp.float32)
        other = other_ref[here, :].astype(jnp.float32)
        total = jnp.sum(own, axis=1, keepdims=True) + jnp.sum(other, axis=1, keepdims=True)
        squares = jnp.sum(own * own, axis=1, keepdims=True) + jnp.sum(
            other * other, axis=1, keepdims=True
        )
        average = total / S
        variance = squares / S - average * average
        scale = lax.rsqrt(variance + epsilon)
        own_out[here, :] = (((own - average) * scale) * 0.03125).astype(jnp.bfloat16)
        other_out[here, :] = (((other - average) * scale) * 0.03125).astype(jnp.bfloat16)


def runs_of(pairs, order):
    found = []
    for j, both in sorted({(j, both) for _, j, both in pairs}):
        places = sorted(order.index(i) for i, q, t in pairs if (q, t) == (j, both))
        for place in places:
            if found and found[-1][0] == j and found[-1][2] == both and found[-1][1][-1] == place - 1:
                found[-1][1].append(place)
            else:
                found.append((j, [place], both))
    return found


def stage_sums(blocks, pairs, first, last, *refs):
    refs = list(refs)
    held = {b: (refs.pop(0), refs.pop(0)) for b in blocks}
    before = None if first else refs.pop(0)
    if last:
        own_ref, keep_ref, give_ref = refs.pop(0), refs.pop(0), refs.pop(0)
    else:
        out_ref = refs.pop(0)
    row_ref, col_ref, right0_ref, right1_ref = refs
    core = lax.axis_index("layer")
    genes = held[blocks[0]][0].shape[0]
    half = genes // 2
    mine = pl.ds(pl.multiple_of(core * half, half), half)
    order = sorted({i for i, _, _ in pairs})
    for place, i in enumerate(order):
        for right_ref, block_ref in zip((right0_ref, right1_ref), held[i]):
            right_ref[place * half : (place + 1) * half, :] = block_ref[mine, :]
    rows_of = sorted({j for _, j, both in pairs if both})
    begun = set()
    for j, places, both in runs_of(pairs, order):
        wide = pl.ds(places[0] * half, len(places) * half)
        t = sum(
            lax.dot_general(
                left_ref[...],
                right_ref[wide, :],
                (((1,), (1,)), ((), ())),
                preferred_element_type=jnp.float32,
            )
            for left_ref, right_ref in zip(held[j], (right0_ref, right1_ref))
        )
        t = 1.0 + t
        t = t * t
        t = t * t
        t = t * t * t
        cols = jnp.sum(t.reshape(genes // 8, 8, t.shape[1]), axis=0)
        for k, place in enumerate(places):
            part = cols[:, k * half : (k + 1) * half]
            if ("c", place) in begun:
                col_ref[place] += part
            else:
                col_ref[place] = part
                begun.add(("c", place))
        if both:
            r = rows_of.index(j)
            full = t.shape[1] // 128 * 128
            part = sum(t[:, q : q + 128] for q in range(0, full, 128))
            if ("r", j) in begun:
                row_ref[r] += part
            else:
                row_ref[r] = part
                begun.add(("r", j))
            if full < t.shape[1]:
                row_ref[r, :, : t.shape[1] - full] += t[:, full:]
    ones = jnp.ones((8, 128), jnp.float32)
    for b in range(BLOCKS):
        parts = [jnp.zeros((1, half), jnp.float32)] * 2
        if before is not None:
            parts = [before[h, pl.ds(b, 1), :] for h in range(2)]
        if b in rows_of:
            rows = lax.dot_general(
                ones,
                row_ref[rows_of.index(b)],
                (((1,), (1,)), ((), ())),
                precision=lax.Precision.HIGHEST,
                preferred_element_type=jnp.float32,
            )
            parts = [p + rows[:1, h * half : (h + 1) * half] for h, p in enumerate(parts)]
        if b in order:
            cols = jnp.sum(col_ref[order.index(b)], axis=0, keepdims=True)
            parts = [p + jnp.where(core == h, cols, 0.0) for h, p in enumerate(parts)]
        for h in range(2):
            if not last:
                out_ref[h, pl.ds(b, 1), :] = parts[h]
            elif b == 0:
                own_ref[pl.ds(h, 1), :] = parts[h] * (0.5**12)
            else:
                kept = jnp.where(core == (b - 1) // 5, 1.0, 0.0) * (0.5**12)
                row = pl.ds((b - 1) % 5, 1)
                if b <= 5:
                    keep_ref[h, row, :] = parts[h] * kept
                    give_ref[h, row, :] = parts[h] * (0.5**12 - kept)
                else:
                    keep_ref[h, row, :] += parts[h] * kept
                    give_ref[h, row, :] += parts[h] * (0.5**12 - kept)


def joined_sums(keep_ref, got_ref, *out_refs):
    for m, out_ref in enumerate(out_refs):
        for h in range(2):
            row = pl.ds(m, 1)
            out_ref[pl.ds(h, 1), :] = keep_ref[h, row, :] + got_ref[h, row, :]


def owner_sums(own_ref, *refs):
    *arrived, mine_ref, other_ref = refs
    total = own_ref[...]
    for ref in arrived:
        total += ref[...]
    first = lax.axis_index("layer") == 0
    mine_ref[...] = jnp.where(first, total[:1], total[1:])
    other_ref[...] = jnp.where(first, total[1:], total[:1])


STAGES = ((0, 1, 2, 3, 4), (5, 6, 7), (8, 9, 10))


def all_sums(held, genes):
    half = genes // 2
    vmem = pl.BlockSpec(memory_space=pltpu.VMEM)
    done = []
    for number, new in enumerate(STAGES):
        first, last = number == 0, number == len(STAGES) - 1
        pairs = [p for p in PAIRS if max(p[:2]) in new]
        blocks = sorted({b for p in pairs for b in p[:2]})
        args = [h for b in blocks for h in held[b]] + done
        out_shape = [jax.ShapeDtypeStruct((2, 16, half), jnp.float32)]
        if last:
            out_shape = [jax.ShapeDtypeStruct((2, half), jnp.float32)]
            out_shape += [jax.ShapeDtypeStruct((2, 8, half), jnp.float32)] * 2
        right = len({i for i, _, _ in pairs})
        call = pl.pallas_call(
            functools.partial(stage_sums, tuple(blocks), tuple(pairs), first, last),
            out_shape=out_shape,
            in_specs=[vmem] * len(args),
            out_specs=[vmem] * len(out_shape),
            scratch_shapes=[
                pltpu.VMEM((len({j for _, j, both in pairs if both}), genes, 128), jnp.float32),
                pltpu.VMEM((right, 8, half), jnp.float32),
                pltpu.VMEM((right * half, S // 2), jnp.bfloat16),
                pltpu.VMEM((right * half, S // 2), jnp.bfloat16),
            ],
            compiler_params=pltpu.CompilerParams(vmem_limit_bytes=VMEM_BYTES),
            cost_estimate=pl.CostEstimate(
                flops=len(pairs) * genes * genes * S, bytes_accessed=2**20, transcendentals=0
            ),
        )
        done = list(call(*args))
    return done


def small(body, results, limit=2**20):
    vmem = pl.BlockSpec(memory_space=pltpu.VMEM)
    return pl.pallas_call(
        body,
        out_shape=[jax.ShapeDtypeStruct(r.shape, r.dtype) for r in results],
        out_specs=[vmem] * len(results),
        compiler_params=pltpu.CompilerParams(vmem_limit_bytes=limit),
    )


def on_device(expression):
    genes, _ = expression.shape
    other = fetch(expression, (0, 0, 0), 1)
    held = [small(standardize, [expression] * 2, 8 * 2**20)(expression, other)]
    got = {DELTA[0]: held[0][0]}
    for b, (d, parent) in enumerate(OFFSETS):
        if b == 0:
            continue
        source = DELTA[0] if parent is None else parent
        got[d] = fetch(got[source], minus(d, source))
        held.append((got[d], fetch(got[d], (0, 0, 0), 1)))
    own, keep, give = all_sums(held, genes)
    got = fetch(give, (0, 0, 0), 1)
    joined = small(joined_sums, [own] * 5)(keep, got)
    arrived = [deliver(v, DELTA[1 + m], DELTA[6 + m]) for m, v in enumerate(joined)]
    mine, other = small(owner_sums, [own[:1]] * 2)(own, *arrived)
    return (mine + fetch(other, (0, 0, 0), 1)).reshape(genes // 2) - 1.0


def solution(mesh):
    torus = Mesh(mesh.devices.reshape(2, N, N, 2, 2), ALL)

    return jax.shard_map(
        on_device, mesh=torus, in_specs=(P(CHIP, "layer"),), out_specs=P(ALL), check_vma=False
    )
```

```python
import functools
import itertools

import jax
import jax.numpy as jnp
from jax import lax
from jax.experimental import pallas as pl
from jax.experimental.pallas import tpu as pltpu
from jax.sharding import Mesh
from jax.sharding import PartitionSpec as P


S = 1024
N = 4
CHIP = ("x_hi", "z", "y", "x_lo")
ALL = CHIP + ("layer",)
epsilon = 1e-05
VMEM_BYTES = 16 * 2**20


OFFSETS = (
    ((0, 0, 0), None),
    ((0, 3, 0), None),
    ((3, 1, 0), None),
    ((1, 0, 3), None),
    ((0, 0, 1), None),
    ((0, 3, 2), (0, 3, 0)),
    ((3, 1, 3), (3, 1, 0)),
    ((2, 0, 3), (1, 0, 3)),
    ((2, 1, 0), (3, 1, 0)),
    ((0, 3, 1), (0, 0, 1)),
    ((0, 1, 0), None),
)
STAGES = ((0, 1, 2, 3, 4), (7,), (8, 9), (10, 5), (6,))
SENDS = ((6, 7), (5, 8), (2, 3), (9, 1), (4, 10))
DELTA = tuple(d for d, _ in OFFSETS)
BLOCKS = len(DELTA)


def minus(a, b):
    return tuple((p - q) % N for p, q in zip(a, b))


def choose_pairs():
    pairs, done = [(0, 0, False)], {(0, 0, 0)}
    order = [b for new in STAGES for b in new]
    for i, j in ((i, j) for k, j in enumerate(order) for i in order[:k]):
        d = minus(DELTA[i], DELTA[j])
        if d not in done:
            e = minus((0, 0, 0), d)
            done |= {d, e}
            pairs.append((i, j, d != e))
    assert len(done) == N**3
    return tuple(pairs)


PAIRS = choose_pairs()


def place(x, y, z, c):
    return (((x // 2 * N + z) * N + y) * 2 + x % 2) * 2 + c


def chips():
    return itertools.product(range(N), range(N), range(N))


def fetch(value, d, flip=0):
    pairs = []
    for p in chips():
        q = tuple((a + b) % N for a, b in zip(p, d))
        for c in range(2):
            pairs.append((place(*q, c ^ flip), place(*p, c)))
    return lax.ppermute(value, ALL, pairs)


def deliver(value, d0, d1):
    pairs = []
    for p in chips():
        for c, d in enumerate((d0, d1)):
            q = tuple((a + b) % N for a, b in zip(p, d))
            pairs.append((place(*p, c), place(*q, c)))
    return lax.ppermute(value, ALL, pairs)


def bring(in_ref, out_ref):
    out_ref[...] = in_ref[...]


def standardize(own_ref, other_ref, own_out, other_out):
    rows = 32
    for r in range(0, own_ref.shape[0], rows):
        here = pl.ds(r, rows)
        own = own_ref[here, :].astype(jnp.float32)
        other = other_ref[here, :].astype(jnp.float32)
        total = jnp.sum(own, axis=1, keepdims=True) + jnp.sum(other, axis=1, keepdims=True)
        squares = jnp.sum(own * own, axis=1, keepdims=True) + jnp.sum(
            other * other, axis=1, keepdims=True
        )
        average = total / S
        variance = squares / S - average * average
        scale = lax.rsqrt(variance + epsilon)
        own_out[here, :] = (((own - average) * scale) * 0.03125).astype(jnp.bfloat16)
        other_out[here, :] = (((other - average) * scale) * 0.03125).astype(jnp.bfloat16)


def runs_of(pairs, order):
    found = []
    for j, both in sorted({(j, both) for _, j, both in pairs}):
        places = sorted(order.index(i) for i, q, t in pairs if (q, t) == (j, both))
        for place in places:
            if found and found[-1][0] == j and found[-1][2] == both and found[-1][1][-1] == place - 1:
                found[-1][1].append(place)
            else:
                found.append((j, [place], both))
    return found


def stage_sums(blocks, pairs, first, last, *refs):
    refs = list(refs)
    held = {b: (refs.pop(0), refs.pop(0)) for b in blocks}
    before = None if first else refs.pop(0)
    if last:
        own_ref, keep_ref, give_ref = refs.pop(0), refs.pop(0), refs.pop(0)
    else:
        out_ref = refs.pop(0)
    row_ref, col_ref, right0_ref, right1_ref = refs
    core = lax.axis_index("layer")
    genes = held[blocks[0]][0].shape[0]
    half = genes // 2
    mine = pl.ds(pl.multiple_of(core * half, half), half)
    order = sorted({i for i, _, _ in pairs})
    for place, i in enumerate(order):
        for right_ref, block_ref in zip((right0_ref, right1_ref), held[i]):
            right_ref[place * half : (place + 1) * half, :] = block_ref[mine, :]
    rows_of = sorted({j for _, j, both in pairs if both})
    begun = set()
    for j, places, both in runs_of(pairs, order):
        wide = pl.ds(places[0] * half, len(places) * half)
        t = sum(
            lax.dot_general(
                left_ref[...],
                right_ref[wide, :],
                (((1,), (1,)), ((), ())),
                preferred_element_type=jnp.float32,
            )
            for left_ref, right_ref in zip(held[j], (right0_ref, right1_ref))
        )
        t = 1.0 + t
        t = t * t
        t = t * t
        t = t * t * t
        cols = jnp.sum(t.reshape(genes // 8, 8, t.shape[1]), axis=0)
        for k, place in enumerate(places):
            part = cols[:, k * half : (k + 1) * half]
            if ("c", place) in begun:
                col_ref[place] += part
            else:
                col_ref[place] = part
                begun.add(("c", place))
        if both:
            r = rows_of.index(j)
            full = t.shape[1] // 128 * 128
            part = sum(t[:, q : q + 128] for q in range(0, full, 128))
            if ("r", j) in begun:
                row_ref[r] += part
            else:
                row_ref[r] = part
                begun.add(("r", j))
            if full < t.shape[1]:
                row_ref[r, :, : t.shape[1] - full] += t[:, full:]
    ones = jnp.ones((8, 128), jnp.float32)
    late = []
    for b in range(BLOCKS):
        parts = [jnp.zeros((1, half), jnp.float32)] * 2
        if before is not None:
            parts = [before[h, pl.ds(b, 1), :] for h in range(2)]
        if b in rows_of:
            rows = lax.dot_general(
                ones,
                row_ref[rows_of.index(b)],
                (((1,), (1,)), ((), ())),
                precision=lax.Precision.HIGHEST,
                preferred_element_type=jnp.float32,
            )
            parts = [p + rows[:1, h * half : (h + 1) * half] for h, p in enumerate(parts)]
        if b in order:
            cols = jnp.sum(col_ref[order.index(b)], axis=0, keepdims=True)
            parts = [p + jnp.where(core == h, cols, 0.0) for h, p in enumerate(parts)]
        for h in range(2):
            if not last:
                out_ref[h, pl.ds(b, 1), :] = parts[h]
            elif b == 0:
                own_ref[pl.ds(h, 1), :] = parts[h] * (0.5**12)
            else:
                (m, side), *_ = [(m, pair.index(b)) for m, pair in enumerate(SENDS) if b in pair]
                kept = jnp.where(core == side, 1.0, 0.0) * (0.5**12)
                row = pl.ds(m, 1)
                if side == 0:
                    keep_ref[h, row, :] = parts[h] * kept
                    give_ref[h, row, :] = parts[h] * (0.5**12 - kept)
                else:
                    late.append((h, row, parts[h] * kept, parts[h] * (0.5**12 - kept)))
    if last:
        for h, row, kept, given in late:
            keep_ref[h, row, :] += kept
            give_ref[h, row, :] += given


def joined_sums(keep_ref, got_ref, *out_refs):
    for m, out_ref in enumerate(out_refs):
        for h in range(2):
            row = pl.ds(m, 1)
            out_ref[pl.ds(h, 1), :] = keep_ref[h, row, :] + got_ref[h, row, :]


def owner_sums(own_ref, *refs):
    *arrived, mine_ref, other_ref = refs
    total = own_ref[...]
    for ref in arrived:
        total += ref[...]
    first = lax.axis_index("layer") == 0
    mine_ref[...] = jnp.where(first, total[:1], total[1:])
    other_ref[...] = jnp.where(first, total[1:], total[:1])


def all_sums(held, genes):
    half = genes // 2
    vmem = pl.BlockSpec(memory_space=pltpu.VMEM)
    done = []
    for number, new in enumerate(STAGES):
        first, last = number == 0, number == len(STAGES) - 1
        pairs = [p for p in PAIRS if p[1] in new]
        blocks = sorted({b for p in pairs for b in p[:2]})
        args = [h for b in blocks for h in held[b]] + done
        out_shape = [jax.ShapeDtypeStruct((2, 16, half), jnp.float32)]
        if last:
            out_shape = [jax.ShapeDtypeStruct((2, half), jnp.float32)]
            out_shape += [jax.ShapeDtypeStruct((2, 8, half), jnp.float32)] * 2
        right = len({i for i, _, _ in pairs})
        call = pl.pallas_call(
            functools.partial(stage_sums, tuple(blocks), tuple(pairs), first, last),
            out_shape=out_shape,
            in_specs=[vmem] * len(args),
            out_specs=[vmem] * len(out_shape),
            scratch_shapes=[
                pltpu.VMEM((len({j for _, j, both in pairs if both}), genes, 128), jnp.float32),
                pltpu.VMEM((right, 8, half), jnp.float32),
                pltpu.VMEM((right * half, S // 2), jnp.bfloat16),
                pltpu.VMEM((right * half, S // 2), jnp.bfloat16),
            ],
            compiler_params=pltpu.CompilerParams(vmem_limit_bytes=VMEM_BYTES),
            cost_estimate=pl.CostEstimate(
                flops=len(pairs) * genes * genes * S, bytes_accessed=2**20, transcendentals=0
            ),
        )
        done = list(call(*args))
    return done


def small(body, results, limit=2**20):
    vmem = pl.BlockSpec(memory_space=pltpu.VMEM)
    return pl.pallas_call(
        body,
        out_shape=[jax.ShapeDtypeStruct(r.shape, r.dtype) for r in results],
        out_specs=[vmem] * len(results),
        compiler_params=pltpu.CompilerParams(vmem_limit_bytes=limit),
    )


def on_device(expression):
    genes, _ = expression.shape
    other = fetch(expression, (0, 0, 0), 1)
    (expression,) = small(bring, [expression], 4 * 2**20)(expression)
    held = [small(standardize, [expression] * 2, 8 * 2**20)(expression, other)]
    got = {DELTA[0]: held[0][0]}
    for b, (d, parent) in enumerate(OFFSETS):
        if b == 0:
            continue
        source = DELTA[0] if parent is None else parent
        got[d] = fetch(got[source], minus(d, source))
        held.append((got[d], fetch(got[d], (0, 0, 0), 1)))
    own, keep, give = all_sums(held, genes)
    got = fetch(give, (0, 0, 0), 1)
    joined = small(joined_sums, [own] * len(SENDS))(keep, got)
    arrived = []
    for m, (b0, b1) in enumerate(SENDS):
        arrived.append(deliver(joined[m], DELTA[b0], DELTA[b1]))
    mine, other = small(owner_sums, [own[:1]] * 2)(own, *arrived)
    return (mine + fetch(other, (0, 0, 0), 1)).reshape(genes // 2) - 1.0


def solution(mesh):
    torus = Mesh(mesh.devices.reshape(2, N, N, 2, 2), ALL)

    return jax.shard_map(
        on_device, mesh=torus, in_specs=(P(CHIP, "layer"),), out_specs=P(ALL), check_vma=False
    )
```

```python
import functools
import itertools

import jax
import jax.numpy as jnp
from jax import lax
from jax.experimental import pallas as pl
from jax.experimental.pallas import tpu as pltpu
from jax.sharding import Mesh
from jax.sharding import PartitionSpec as P


S = 1024
N = 4
CHIP = ("x_hi", "z", "y", "x_lo")
ALL = CHIP + ("layer",)
epsilon = 1e-05
VMEM_BYTES = 16 * 2**20


OFFSETS = (
    ((0, 0, 0), None),
    ((3, 3, 3), None),
    ((1, 0, 0), None),
    ((0, 1, 0), None),
    ((3, 0, 1), None),
    ((1, 0, 1), (1, 0, 0)),
    ((1, 0, 3), (1, 0, 0)),
    ((0, 2, 0), (0, 1, 0)),
    ((0, 3, 3), (3, 3, 3)),
    ((3, 2, 3), (3, 3, 3)),
    ((2, 0, 1), (3, 0, 1)),
)
STAGES = ((0, 1, 2, 3, 4), (5,), (6, 7), (8, 9), (10,))
SENDS = ((9, 10), (1, 8), (7, 4), (5, 6), (2, 3))
DELTA = tuple(d for d, _ in OFFSETS)
BLOCKS = len(DELTA)


def minus(a, b):
    return tuple((p - q) % N for p, q in zip(a, b))


def choose_pairs():
    pairs, done = [(0, 0, False)], {(0, 0, 0)}
    order = [b for new in STAGES for b in new]
    for i, j in ((i, j) for k, j in enumerate(order) for i in order[:k]):
        d = minus(DELTA[i], DELTA[j])
        if d not in done:
            e = minus((0, 0, 0), d)
            done |= {d, e}
            pairs.append((i, j, d != e))
    assert len(done) == N**3
    return tuple(pairs)


PAIRS = choose_pairs()


def place(x, y, z, c):
    return (((x // 2 * N + z) * N + y) * 2 + x % 2) * 2 + c


def chips():
    return itertools.product(range(N), range(N), range(N))


def fetch(value, d, flip=0):
    pairs = []
    for p in chips():
        q = tuple((a + b) % N for a, b in zip(p, d))
        for c in range(2):
            pairs.append((place(*q, c ^ flip), place(*p, c)))
    return lax.ppermute(value, ALL, pairs)


def deliver(value, d0, d1):
    pairs = []
    for p in chips():
        for c, d in enumerate((d0, d1)):
            q = tuple((a + b) % N for a, b in zip(p, d))
            pairs.append((place(*p, c), place(*q, c)))
    return lax.ppermute(value, ALL, pairs)


def bring(in_ref, out_ref):
    out_ref[...] = in_ref[...]


def standardize(own_ref, other_ref, own_out, other_out):
    rows = 32
    for r in range(0, own_ref.shape[0], rows):
        here = pl.ds(r, rows)
        own = own_ref[here, :].astype(jnp.float32)
        other = other_ref[here, :].astype(jnp.float32)
        total = jnp.sum(own, axis=1, keepdims=True) + jnp.sum(other, axis=1, keepdims=True)
        squares = jnp.sum(own * own, axis=1, keepdims=True) + jnp.sum(
            other * other, axis=1, keepdims=True
        )
        average = total / S
        variance = squares / S - average * average
        scale = lax.rsqrt(variance + epsilon)
        own_out[here, :] = (((own - average) * scale) * 0.03125).astype(jnp.bfloat16)
        other_out[here, :] = (((other - average) * scale) * 0.03125).astype(jnp.bfloat16)


def runs_of(pairs, order):
    found = []
    for j, both in sorted({(j, both) for _, j, both in pairs}):
        places = sorted(order.index(i) for i, q, t in pairs if (q, t) == (j, both))
        for place in places:
            if found and found[-1][0] == j and found[-1][2] == both and found[-1][1][-1] == place - 1:
                found[-1][1].append(place)
            else:
                found.append((j, [place], both))
    return found


def stage_sums(blocks, pairs, first, last, *refs):
    refs = list(refs)
    held = {b: (refs.pop(0), refs.pop(0)) for b in blocks}
    before = None if first else refs.pop(0)
    if last:
        own_ref, keep_ref, give_ref = refs.pop(0), refs.pop(0), refs.pop(0)
    else:
        out_ref = refs.pop(0)
    row_ref, col_ref, right0_ref, right1_ref = refs
    core = lax.axis_index("layer")
    genes = held[blocks[0]][0].shape[0]
    half = genes // 2
    mine = pl.ds(pl.multiple_of(core * half, half), half)
    order = sorted({i for i, _, _ in pairs})
    for place, i in enumerate(order):
        for right_ref, block_ref in zip((right0_ref, right1_ref), held[i]):
            right_ref[place * half : (place + 1) * half, :] = block_ref[mine, :]
    rows_of = sorted({j for _, j, both in pairs if both})
    begun = set()
    for j, places, both in runs_of(pairs, order):
        wide = pl.ds(places[0] * half, len(places) * half)
        t = sum(
            lax.dot_general(
                left_ref[...],
                right_ref[wide, :],
                (((1,), (1,)), ((), ())),
                preferred_element_type=jnp.float32,
            )
            for left_ref, right_ref in zip(held[j], (right0_ref, right1_ref))
        )
        t = 1.0 + t
        t = t * t
        t = t * t
        t = t * t * t
        cols = jnp.sum(t.reshape(genes // 8, 8, t.shape[1]), axis=0)
        for k, place in enumerate(places):
            part = cols[:, k * half : (k + 1) * half]
            if ("c", place) in begun:
                col_ref[place] += part
            else:
                col_ref[place] = part
                begun.add(("c", place))
        if both:
            r = rows_of.index(j)
            full = t.shape[1] // 128 * 128
            part = sum(t[:, q : q + 128] for q in range(0, full, 128))
            if ("r", j) in begun:
                row_ref[r] += part
            else:
                row_ref[r] = part
                begun.add(("r", j))
            if full < t.shape[1]:
                row_ref[r, :, : t.shape[1] - full] += t[:, full:]
    ones = jnp.ones((8, 128), jnp.float32)
    late = []
    for b in range(BLOCKS):
        parts = [jnp.zeros((1, half), jnp.float32)] * 2
        if before is not None:
            parts = [before[h, pl.ds(b, 1), :] for h in range(2)]
        if b in rows_of:
            rows = lax.dot_general(
                ones,
                row_ref[rows_of.index(b)],
                (((1,), (1,)), ((), ())),
                precision=lax.Precision.HIGHEST,
                preferred_element_type=jnp.float32,
            )
            parts = [p + rows[:1, h * half : (h + 1) * half] for h, p in enumerate(parts)]
        if b in order:
            cols = jnp.sum(col_ref[order.index(b)], axis=0, keepdims=True)
            parts = [p + jnp.where(core == h, cols, 0.0) for h, p in enumerate(parts)]
        for h in range(2):
            if not last:
                out_ref[h, pl.ds(b, 1), :] = parts[h]
            elif b == 0:
                own_ref[pl.ds(h, 1), :] = parts[h] * (0.5**12)
            else:
                (m, side), *_ = [(m, pair.index(b)) for m, pair in enumerate(SENDS) if b in pair]
                kept = jnp.where(core == side, 1.0, 0.0) * (0.5**12)
                row = pl.ds(m, 1)
                if side == 0:
                    keep_ref[h, row, :] = parts[h] * kept
                    give_ref[h, row, :] = parts[h] * (0.5**12 - kept)
                else:
                    late.append((h, row, parts[h] * kept, parts[h] * (0.5**12 - kept)))
    if last:
        for h, row, kept, given in late:
            keep_ref[h, row, :] += kept
            give_ref[h, row, :] += given


def joined_sums(keep_ref, got_ref, *out_refs):
    for m, out_ref in enumerate(out_refs):
        for h in range(2):
            row = pl.ds(m, 1)
            out_ref[pl.ds(h, 1), :] = keep_ref[h, row, :] + got_ref[h, row, :]


def owner_sums(own_ref, *refs):
    *arrived, mine_ref, other_ref = refs
    total = own_ref[...]
    for ref in arrived:
        total += ref[...]
    first = lax.axis_index("layer") == 0
    mine_ref[...] = jnp.where(first, total[:1], total[1:])
    other_ref[...] = jnp.where(first, total[1:], total[:1])


def all_sums(held, genes):
    half = genes // 2
    vmem = pl.BlockSpec(memory_space=pltpu.VMEM)
    done = []
    for number, new in enumerate(STAGES):
        first, last = number == 0, number == len(STAGES) - 1
        pairs = [p for p in PAIRS if p[1] in new]
        blocks = sorted({b for p in pairs for b in p[:2]})
        args = [h for b in blocks for h in held[b]] + done
        out_shape = [jax.ShapeDtypeStruct((2, 16, half), jnp.float32)]
        if last:
            out_shape = [jax.ShapeDtypeStruct((2, half), jnp.float32)]
            out_shape += [jax.ShapeDtypeStruct((2, 8, half), jnp.float32)] * 2
        right = len({i for i, _, _ in pairs})
        call = pl.pallas_call(
            functools.partial(stage_sums, tuple(blocks), tuple(pairs), first, last),
            out_shape=out_shape,
            in_specs=[vmem] * len(args),
            out_specs=[vmem] * len(out_shape),
            scratch_shapes=[
                pltpu.VMEM((len({j for _, j, both in pairs if both}), genes, 128), jnp.float32),
                pltpu.VMEM((right, 8, half), jnp.float32),
                pltpu.VMEM((right * half, S // 2), jnp.bfloat16),
                pltpu.VMEM((right * half, S // 2), jnp.bfloat16),
            ],
            compiler_params=pltpu.CompilerParams(vmem_limit_bytes=VMEM_BYTES),
            cost_estimate=pl.CostEstimate(
                flops=len(pairs) * genes * genes * S, bytes_accessed=2**20, transcendentals=0
            ),
        )
        done = list(call(*args))
    return done


def small(body, results, limit=2**20):
    vmem = pl.BlockSpec(memory_space=pltpu.VMEM)
    return pl.pallas_call(
        body,
        out_shape=[jax.ShapeDtypeStruct(r.shape, r.dtype) for r in results],
        out_specs=[vmem] * len(results),
        compiler_params=pltpu.CompilerParams(vmem_limit_bytes=limit),
    )


def on_device(expression):
    genes, _ = expression.shape
    other = fetch(expression, (0, 0, 0), 1)
    (expression,) = small(bring, [expression], 4 * 2**20)(expression)
    held = [small(standardize, [expression] * 2, 8 * 2**20)(expression, other)]
    got = {DELTA[0]: held[0][0]}
    for b, (d, parent) in enumerate(OFFSETS):
        if b == 0:
            continue
        source = DELTA[0] if parent is None else parent
        got[d] = fetch(got[source], minus(d, source))
        held.append((got[d], fetch(got[d], (0, 0, 0), 1)))
    own, keep, give = all_sums(held, genes)
    got = fetch(give, (0, 0, 0), 1)
    joined = small(joined_sums, [own] * len(SENDS))(keep, got)
    arrived = []
    for m, (b0, b1) in enumerate(SENDS):
        arrived.append(deliver(joined[m], DELTA[b0], DELTA[b1]))
    mine, other = small(owner_sums, [own[:1]] * 2)(own, *arrived)
    return (mine + fetch(other, (0, 0, 0), 1)).reshape(genes // 2) - 1.0


def solution(mesh):
    torus = Mesh(mesh.devices.reshape(2, N, N, 2, 2), ALL)

    return jax.shard_map(
        on_device, mesh=torus, in_specs=(P(CHIP, "layer"),), out_specs=P(ALL), check_vma=False
    )
```
